32 devices in a mesh: tm: 8 (over z, y), coef: 4 (over x, core).
Axes of the slice: x: 2, y: 2, z: 4, core: 2. Of those that a mesh axis runs over, the one named last changes fastest.
Arguments:
- design: bfloat16 [2048, 50176], P('tm', 'coef'), may hold values from -0.0390625 to 0.0390625
- observed: float32 [2048, 128], P('tm'), may hold values from -6 to 6
- slab_counts: int32 [8], P('tm'), may hold values from 128 to 256, as said below
- gap_mask: int32 [2048], P('tm'), may hold values 0 or 1
- filter_taps: float32 [128], replicated, may hold values from -0.5 to 1.2, as said below
- kaula_diag: float32 [50176], P('coef'), may hold values from 0.1 to 1
- precond: float32 [50176], P('coef'), may hold values from 0.3 to 3
Outputs:
- solution: float32 [50176, 128], P(('coef', 'tm'))
- residual: float32 [50176, 128], P(('coef', 'tm'))
The draws below stay inside these ranges and needn't reach their ends.
Inputs may be any that keep to these rules, and one draw needn't show every extreme that they name: `slab_counts`: every slab holds at most 256 valid epochs, and some slab holds exactly 256. filter_taps[0] lies between 1 and 1.2.
All inputs are finite; a program needn't handle non-finite values. No bound on the sum of `gap_mask` on one device may be relied on, other than what follows from the above.
Results may differ from the reference program's by a relative error of at most 0.0065.
The reference program's roundings to bfloat16 on the way (of `weighted`) count: a program that leaves them out, or rounds other values in their place, can miss the bound.
Values may be sent and summed in bfloat16 or wider, within the bound.
No kernel may reach another device: no remote copies, remote signals or barrier semaphores. Data moves between devices by JAX's collectives and lax.ppermute only.
A program may use at most 64 MiB of HBM per device.

```python
import math
import jax
import jax.numpy as jnp
from jax import lax

NC = 50176
R = 128
E_DEV = 256
BAND = 128
ITERS = 2
EPOCHS = 2048
N_TM = 8


def draw_slab_counts(key, part):
    first_key = jax.random.fold_in(key, 11)
    second_key = jax.random.fold_in(key, 12)
    values = jax.random.randint(first_key, (N_TM,), E_DEV // 2, E_DEV + 1)
    chosen = jax.random.randint(second_key, (), 0, N_TM)
    return jnp.where(jnp.arange(N_TM) == chosen, E_DEV, values).astype(jnp.int32)


def draw_filter_taps(key, part):
    first_key = jax.random.fold_in(key, 21)
    second_key = jax.random.fold_in(key, 22)
    lags = jnp.arange(BAND).astype(jnp.float32)
    decay = jnp.exp(-1.5 * lags / BAND)
    noise = 0.12 * jnp.clip(jax.random.normal(first_key, (BAND,), jnp.float32), -4.0, 4.0)
    leading = 1.0 + 0.2 * jax.random.uniform(second_key, (BAND,), jnp.float32)
    return jnp.where(lags == 0.0, leading, decay * noise).astype(jnp.float32)


def plant(values, rng, smallest, high):
    place = [jax.random.randint(jax.random.fold_in(rng, axis), (), 0, length) for axis, length in enumerate(values.shape)]
    widest = values.shape.index(max(values.shape))
    next_to = place[:widest] + [(place[widest] + 1) % values.shape[widest]] + place[widest + 1:]
    return values.at[tuple(place)].set(smallest).at[tuple(next_to)].set(high)


def with_spikes(drawn, rng, source, target, parts, factor):
    def block_of(dim):
        return (jnp.arange(drawn.shape[dim]) // (drawn.shape[dim] // parts)).reshape((-1,) + (1,) * (drawn.ndim - 1 - dim))

    one_side = jax.random.permutation(rng, parts)[block_of(target)]
    second = (block_of(target) + parts // 2) % parts
    return jnp.where((block_of(source) == one_side) | (block_of(source) == second), factor * drawn, drawn)


def shard_levels(stream_key, extent, split, low, top_value):
    factor_of, own = 1.0, jax.random.fold_in(stream_key, 6)
    for axis_at, parts in split:
        heights = jnp.exp(jax.random.uniform(jax.random.fold_in(own, axis_at), (parts,), jnp.float32, low / len(split), top_value / len(split)))
        factor_of = factor_of * jnp.repeat(heights, extent[axis_at] // parts).reshape([-1 if axis == axis_at else 1 for axis in range(len(extent))])
    return factor_of


def centred(own_key, dims, scale, reach, pieces=(), kind=jnp.bfloat16):
    values = scale * jax.random.normal(own_key, dims, jnp.float32)
    if pieces:
        values = values * shard_levels(own_key, dims, pieces, -0.22, 0.18)
    return jnp.clip(values, -reach, reach).astype(kind)


def noise_with(rng, dims, scale, reach, split, heavy, held_as=jnp.bfloat16):
    values = scale * jax.random.normal(rng, dims, jnp.float32)
    if split:
        values = values * shard_levels(rng, dims, split, -0.22, 0.18)
    return jnp.clip(with_spikes(values, jax.random.fold_in(rng, 3), *heavy), -reach, reach).astype(held_as)


def setup_inputs(seed: int = 0) -> dict:
    key_list = jax.random.split(jax.random.key(seed), 8)
    return {
        "design": noise_with(key_list[0], (EPOCHS, NC), NC ** -0.5, 0.0390625, ((0, 8), (1, 4)), (0, 1, 8, 2.0)),
        "observed": centred(key_list[1], (EPOCHS, R), 1.0, 6.0, ((0, 8),), jnp.float32),
        "slab_counts": draw_slab_counts(jax.random.fold_in(key_list[7], 71), 0),
        "gap_mask": plant((jax.random.randint(key_list[3], (EPOCHS,), 0, 8) < 7).astype(jnp.int32), jax.random.fold_in(key_list[3], 1), 0, 1),
        "filter_taps": draw_filter_taps(jax.random.fold_in(key_list[7], 71), 0),
        "kaula_diag": jnp.clip(jnp.exp(math.log(1.0) - 2.3025851 * jax.random.uniform(key_list[5], (NC,), jnp.float32) ** shard_levels(key_list[5], (NC,), ((0, 4),), -0.2, 0.2)), 0.1, 1.0),
        "precond": jnp.clip(jnp.exp(math.log(3.0) - 2.3025851 * jax.random.uniform(key_list[6], (NC,), jnp.float32) ** shard_levels(key_list[6], (NC,), ((0, 4),), -0.2, 0.2)), 0.3, 3.0),
    }


def toeplitz(pattern, band_len):
    tiled = jnp.tile(pattern, band_len)[: band_len * (2 * band_len - 1)]
    return tiled.reshape(band_len, 2 * band_len - 1)[:, :band_len]


def block_pair(filter_taps):
    band_len = filter_taps.shape[0]
    spacer = jnp.zeros((band_len,), jnp.float32)
    reversed_taps = filter_taps[:0:-1]
    lower = jnp.concatenate([filter_taps[:1], spacer, reversed_taps])
    upper = jnp.concatenate([jnp.zeros((1,), jnp.float32), reversed_taps, spacer])
    return toeplitz(lower, band_len), toeplitz(upper, band_len)


def forward(values, lower_block, upper_block):
    band_len = lower_block.shape[0]
    blocks = values.reshape(-1, band_len, values.shape[1])
    previous = jnp.concatenate([jnp.zeros_like(blocks[:1]), blocks[:-1]], 0)
    result = jnp.einsum("ij,bjr->bir", lower_block, blocks, precision=lax.Precision.HIGHEST)
    result = result + jnp.einsum("ij,bjr->bir", upper_block, previous, precision=lax.Precision.HIGHEST)
    return result.reshape(values.shape)


def backward(values, lower_block, upper_block):
    band_len = lower_block.shape[0]
    blocks = values.reshape(-1, band_len, values.shape[1])
    following = jnp.concatenate([blocks[1:], jnp.zeros_like(blocks[:1])], 0)
    result = jnp.einsum("ji,bjr->bir", lower_block, blocks, precision=lax.Precision.HIGHEST)
    result = result + jnp.einsum("ji,bjr->bir", upper_block, following, precision=lax.Precision.HIGHEST)
    return result.reshape(values.shape)


def reference(design, observed, slab_counts, gap_mask, filter_taps, kaula_diag, precond):
    lower_block, upper_block = block_pair(filter_taps)
    position = jnp.arange(EPOCHS, dtype=jnp.int32)
    slab_index = position // E_DEV
    weight = ((gap_mask == 1) & (position % E_DEV < slab_counts[slab_index])).astype(jnp.float32)[:, None]

    def weighted(values):
        inner = forward(weight * values, lower_block, upper_block)
        return (weight * backward(inner, lower_block, upper_block)).astype(jnp.bfloat16)

    def transposed(filtered):
        return lax.dot_general(design, filtered, (((0,), (0,)), ((), ())), preferred_element_type=jnp.float32)

    kaula_col = kaula_diag[:, None]
    precond_col = precond[:, None]
    residual = transposed(weighted(observed))
    solution = jnp.zeros_like(residual)
    scaled = precond_col * residual
    direction = scaled
    norm_now = jnp.sum(residual * scaled, 0)
    for iteration in range(ITERS):
        slab_values = jnp.dot(design, direction.astype(jnp.bfloat16), preferred_element_type=jnp.float32)
        image = transposed(weighted(slab_values)) + kaula_col * direction
        step_len = norm_now / jnp.sum(direction * image, 0)
        solution = solution + step_len * direction
        residual = residual - step_len * image
        scaled = precond_col * residual
        norm_next = jnp.sum(residual * scaled, 0)
        direction = scaled + (norm_next / norm_now) * direction
        norm_now = norm_next
    return solution, residual
```

```python
import jax
import jax.numpy as jnp
from jax import lax
from jax.sharding import PartitionSpec as P

ITERS = 2
LANES = 128
BOTH = ("tm", "coef")


def toeplitz(pattern, band_len):
    tiled = jnp.tile(pattern, band_len)[: band_len * (2 * band_len - 1)]
    return tiled.reshape(band_len, 2 * band_len - 1)[:, :band_len]


def block_pair(filter_taps):
    band_len = filter_taps.shape[0]
    spacer = jnp.zeros((band_len,), jnp.float32)
    reversed_taps = filter_taps[:0:-1]
    lower = jnp.concatenate([filter_taps[:1], spacer, reversed_taps])
    upper = jnp.concatenate([jnp.zeros((1,), jnp.float32), reversed_taps, spacer])
    return (toeplitz(lower, band_len), toeplitz(upper, band_len))


def forward(values, lower_block, upper_block):
    band_len = lower_block.shape[0]
    blocks = values.reshape(-1, band_len, values.shape[1])
    previous = jnp.concatenate([jnp.zeros_like(blocks[:1]), blocks[:-1]], 0)
    result = jnp.einsum("ij,bjr->bir", lower_block, blocks, precision=lax.Precision.HIGHEST)
    result = result + jnp.einsum(
        "ij,bjr->bir", upper_block, previous, precision=lax.Precision.HIGHEST
    )
    return result.reshape(values.shape)


def backward(values, lower_block, upper_block):
    band_len = lower_block.shape[0]
    blocks = values.reshape(-1, band_len, values.shape[1])
    following = jnp.concatenate([blocks[1:], jnp.zeros_like(blocks[:1])], 0)
    result = jnp.einsum("ji,bjr->bir", lower_block, blocks, precision=lax.Precision.HIGHEST)
    result = result + jnp.einsum(
        "ji,bjr->bir", upper_block, following, precision=lax.Precision.HIGHEST
    )
    return result.reshape(values.shape)


def shards(design, observed, slab_counts, gap_mask, filter_taps, kaula_diag, precond):
    epoch_rows, coef_rows = design.shape
    slabs = lax.axis_size("tm")
    owned_rows = coef_rows // slabs
    owner_index = lax.axis_index("tm")

    tile = LANES if coef_rows % LANES == 0 else owned_rows
    tiles = coef_rows // tile
    width = max(
        -(-(slab + 1) * owned_rows // tile) - slab * owned_rows // tile for slab in range(slabs)
    )
    first_tiles = [min(slab * owned_rows // tile, tiles - width) for slab in range(slabs)]
    window = width * tile
    begins = [first * tile for first in first_tiles]
    begin = jnp.array(begins, jnp.int32)[owner_index]
    offset = owner_index * owned_rows - begin

    pieces = jnp.stack([design[:, start : start + window] for start in begins])
    columns = lax.all_to_all(pieces, "tm", 0, 0).reshape(slabs * epoch_rows, window)

    position = jnp.arange(epoch_rows, dtype=jnp.int32)
    own_weight = ((gap_mask == 1) & (position < slab_counts[0])).astype(jnp.float32)
    packed = jnp.concatenate(
        [observed, jnp.broadcast_to(own_weight[:, None], (epoch_rows, LANES))], 1
    )
    packed = lax.all_gather(packed, "tm", axis=0, tiled=True)
    observed_all = packed[:, : observed.shape[1]]
    weight = packed[:, observed.shape[1] : observed.shape[1] + 1]
    lower_block, upper_block = block_pair(filter_taps)

    def weighted(values):
        inner = forward(weight * values, lower_block, upper_block)
        return (weight * backward(inner, lower_block, upper_block)).astype(jnp.bfloat16)

    def transposed(filtered):
        return lax.dot_general(
            columns, filtered, (((0,), (0,)), ((), ())), preferred_element_type=jnp.float32
        )

    def reduced(vector, rows):
        product = jnp.dot(
            columns, vector.astype(jnp.bfloat16), preferred_element_type=jnp.float32
        )
        extra = jnp.stack(rows + [jnp.zeros_like(rows[0])] * (8 - len(rows)))
        total = lax.psum(jnp.concatenate([product, extra]), BOTH)
        return total[: product.shape[0]], [total[product.shape[0] + i] for i in range(len(rows))]

    local = jnp.arange(window, dtype=jnp.int32)
    owned = (local >= offset) & (local < offset + owned_rows)

    def window_of(values):
        cut = lax.dynamic_slice_in_dim(values, begin, window, 0)
        return jnp.where(owned, cut, 0.0)[:, None]

    kaula_col = window_of(kaula_diag)
    precond_col = window_of(precond)

    residual = transposed(weighted(observed_all))
    solution = jnp.zeros_like(residual)
    direction = None
    for iteration in range(ITERS):
        scaled = precond_col * residual
        rows = [jnp.sum(residual * scaled, 0), jnp.sum(kaula_col * scaled * scaled, 0)]
        if iteration:
            rows.append(jnp.sum(kaula_col * scaled * direction, 0))
        product, sums = reduced(scaled, rows)
        if iteration:
            ratio = sums[0] / norm_now
            direction = scaled + ratio * direction
            slab_values = product + ratio * slab_values
            ridge = sums[1] + 2.0 * ratio * sums[2] + ratio * ratio * ridge
        else:
            direction, slab_values, ridge = scaled, product, sums[1]
        norm_now = sums[0]
        filtered = weighted(slab_values)
        curvature = jnp.sum(slab_values * filtered.astype(jnp.float32), 0) + ridge
        image = transposed(filtered) + kaula_col * direction
        step_len = norm_now / curvature
        solution = solution + step_len * direction
        residual = residual - step_len * image
    return tuple(
        lax.dynamic_slice_in_dim(values, offset, owned_rows, 0) for values in (solution, residual)
    )


def solution(mesh):
    placed = (P("tm", "coef"), P("tm", None), P("tm"), P("tm"), P(), P("coef"), P("coef"))
    return jax.shard_map(
        shards,
        mesh=mesh,
        in_specs=placed,
        out_specs=(P(("coef", "tm"), None), P(("coef", "tm"), None)),
        check_vma=False,
    )
```

```python
import jax
import jax.numpy as jnp
from jax import lax
from jax.sharding import PartitionSpec as P

ITERS = 2
LANES = 128


def toeplitz(pattern, band_len):
    tiled = jnp.tile(pattern, band_len)[: band_len * (2 * band_len - 1)]
    return tiled.reshape(band_len, 2 * band_len - 1)[:, :band_len]


def block_pair(filter_taps):
    band_len = filter_taps.shape[0]
    spacer = jnp.zeros((band_len,), jnp.float32)
    reversed_taps = filter_taps[:0:-1]
    lower = jnp.concatenate([filter_taps[:1], spacer, reversed_taps])
    upper = jnp.concatenate([jnp.zeros((1,), jnp.float32), reversed_taps, spacer])
    return (toeplitz(lower, band_len), toeplitz(upper, band_len))


def forward(values, lower_block, upper_block):
    band_len = lower_block.shape[0]
    blocks = values.reshape(-1, band_len, values.shape[1])
    previous = jnp.concatenate([jnp.zeros_like(blocks[:1]), blocks[:-1]], 0)
    result = jnp.einsum("ij,bjr->bir", lower_block, blocks, precision=lax.Precision.HIGHEST)
    result = result + jnp.einsum(
        "ij,bjr->bir", upper_block, previous, precision=lax.Precision.HIGHEST
    )
    return result.reshape(values.shape)


def backward(values, lower_block, upper_block):
    band_len = lower_block.shape[0]
    blocks = values.reshape(-1, band_len, values.shape[1])
    following = jnp.concatenate([blocks[1:], jnp.zeros_like(blocks[:1])], 0)
    result = jnp.einsum("ji,bjr->bir", lower_block, blocks, precision=lax.Precision.HIGHEST)
    result = result + jnp.einsum(
        "ji,bjr->bir", upper_block, following, precision=lax.Precision.HIGHEST
    )
    return result.reshape(values.shape)


def exchanged(value, axis, distance):
    return lax.ppermute(
        value, axis, [(index, index ^ distance) for index in range(lax.axis_size(axis))]
    )


def total_sum(value):
    parts = lax.axis_size("coef")
    own = lax.axis_index("coef")
    blocks = value.reshape(parts, -1, value.shape[1])

    def block(distance):
        return lax.dynamic_index_in_dim(blocks, own ^ distance, 0, keepdims=False)

    received = [exchanged(block(distance), "coef", distance) for distance in range(1, parts)]
    mine = sum(received, block(0))
    distance = 1
    while distance < lax.axis_size("tm"):
        mine = mine + exchanged(mine, "tm", distance)
        distance *= 2
    gathered = [mine] + [exchanged(mine, "coef", distance) for distance in range(1, parts)]
    result = jnp.zeros_like(blocks)
    for distance, part in enumerate(gathered):
        result = lax.dynamic_update_index_in_dim(result, part, own ^ distance, 0)
    return result.reshape(value.shape)


def shards(design, observed, slab_counts, gap_mask, filter_taps, kaula_diag, precond):
    epoch_rows, coef_rows = design.shape
    slabs = lax.axis_size("tm")
    owned_rows = coef_rows // slabs
    owner_index = lax.axis_index("tm")

    tile = LANES if coef_rows % LANES == 0 else owned_rows
    tiles = coef_rows // tile
    width = max(
        -(-(slab + 1) * owned_rows // tile) - slab * owned_rows // tile for slab in range(slabs)
    )
    first_tiles = [min(slab * owned_rows // tile, tiles - width) for slab in range(slabs)]
    window = width * tile
    begins = [first * tile for first in first_tiles]
    begin = jnp.array(begins, jnp.int32)[owner_index]
    offset = owner_index * owned_rows - begin

    pieces = jnp.stack([design[:, start : start + window] for start in begins])
    columns = lax.all_to_all(pieces, "tm", 0, 0).reshape(slabs * epoch_rows, window)

    position = jnp.arange(epoch_rows, dtype=jnp.int32)
    own_weight = ((gap_mask == 1) & (position < slab_counts[0])).astype(jnp.float32)
    columns_count = observed.shape[1]
    weight_rows = own_weight.reshape(-1, columns_count)
    blank = jnp.zeros((-weight_rows.shape[0] % 8, columns_count), jnp.float32)
    packed = lax.all_gather(jnp.concatenate([observed, weight_rows, blank]), "tm", axis=0)
    observed_all = packed[:, :epoch_rows].reshape(-1, columns_count)
    weight = packed[:, epoch_rows : epoch_rows + weight_rows.shape[0]].reshape(-1, 1)
    lower_block, upper_block = block_pair(filter_taps)

    def weighted(values):
        inner = forward(weight * values, lower_block, upper_block)
        return (weight * backward(inner, lower_block, upper_block)).astype(jnp.bfloat16)

    def transposed(filtered):
        return lax.dot_general(
            columns, filtered, (((0,), (0,)), ((), ())), preferred_element_type=jnp.float32
        )

    def reduced(vector, rows):
        product = jnp.dot(
            columns, vector.astype(jnp.bfloat16), preferred_element_type=jnp.float32
        )
        unit = 8 * lax.axis_size("coef")
        spare = -(product.shape[0] + len(rows)) % unit
        extra = jnp.stack(rows + [jnp.zeros_like(rows[0])] * spare)
        total = total_sum(jnp.concatenate([product, extra]))
        return total[: product.shape[0]], [total[product.shape[0] + i] for i in range(len(rows))]

    local = jnp.arange(window, dtype=jnp.int32)
    owned = (local >= offset) & (local < offset + owned_rows)

    def window_of(values):
        cut = lax.dynamic_slice_in_dim(values, begin, window, 0)
        return jnp.where(owned, cut, 0.0)[:, None]

    kaula_col = window_of(kaula_diag)
    precond_col = window_of(precond)

    residual = transposed(weighted(observed_all))
    solution = jnp.zeros_like(residual)
    direction = None
    for iteration in range(ITERS):
        scaled = precond_col * residual
        rows = [jnp.sum(residual * scaled, 0), jnp.sum(kaula_col * scaled * scaled, 0)]
        if iteration:
            rows.append(jnp.sum(kaula_col * scaled * direction, 0))
        product, sums = reduced(scaled, rows)
        if iteration:
            ratio = sums[0] / norm_now
            direction = scaled + ratio * direction
            slab_values = product + ratio * slab_values
            ridge = sums[1] + 2.0 * ratio * sums[2] + ratio * ratio * ridge
        else:
            direction, slab_values, ridge = scaled, product, sums[1]
        norm_now = sums[0]
        filtered = weighted(slab_values)
        curvature = jnp.sum(slab_values * filtered.astype(jnp.float32), 0) + ridge
        image = transposed(filtered) + kaula_col * direction
        step_len = norm_now / curvature
        solution = solution + step_len * direction
        residual = residual - step_len * image
    return tuple(
        lax.dynamic_slice_in_dim(values, offset, owned_rows, 0) for values in (solution, residual)
    )


def solution(mesh):
    placed = (P("tm", "coef"), P("tm", None), P("tm"), P("tm"), P(), P("coef"), P("coef"))
    return jax.shard_map(
        shards,
        mesh=mesh,
        in_specs=placed,
        out_specs=(P(("coef", "tm"), None), P(("coef", "tm"), None)),
        check_vma=False,
    )
```

```python
import jax
import jax.numpy as jnp
from jax import lax
from jax.sharding import PartitionSpec as P

ITERS = 2
LANES = 128


def toeplitz(pattern, band_len):
    tiled = jnp.tile(pattern, band_len)[: band_len * (2 * band_len - 1)]
    return tiled.reshape(band_len, 2 * band_len - 1)[:, :band_len]


def block_pair(filter_taps):
    band_len = filter_taps.shape[0]
    spacer = jnp.zeros((band_len,), jnp.float32)
    reversed_taps = filter_taps[:0:-1]
    lower = jnp.concatenate([filter_taps[:1], spacer, reversed_taps])
    upper = jnp.concatenate([jnp.zeros((1,), jnp.float32), reversed_taps, spacer])
    return (toeplitz(lower, band_len), toeplitz(upper, band_len))


def forward(values, lower_block, upper_block):
    band_len = lower_block.shape[0]
    blocks = values.reshape(-1, band_len, values.shape[1])
    previous = jnp.concatenate([jnp.zeros_like(blocks[:1]), blocks[:-1]], 0)
    result = jnp.einsum("ij,bjr->bir", lower_block, blocks, precision=lax.Precision.HIGHEST)
    result = result + jnp.einsum(
        "ij,bjr->bir", upper_block, previous, precision=lax.Precision.HIGHEST
    )
    return result.reshape(values.shape)


def backward(values, lower_block, upper_block):
    band_len = lower_block.shape[0]
    blocks = values.reshape(-1, band_len, values.shape[1])
    following = jnp.concatenate([blocks[1:], jnp.zeros_like(blocks[:1])], 0)
    result = jnp.einsum("ji,bjr->bir", lower_block, blocks, precision=lax.Precision.HIGHEST)
    result = result + jnp.einsum(
        "ji,bjr->bir", upper_block, following, precision=lax.Precision.HIGHEST
    )
    return result.reshape(values.shape)


def exchanged(value, axis, distance):
    return lax.ppermute(
        value, axis, [(index, index ^ distance) for index in range(lax.axis_size(axis))]
    )


def total_sum(value):
    parts = lax.axis_size("coef")
    own = lax.axis_index("coef")
    blocks = value.reshape(parts, -1, value.shape[1])

    def block(distance):
        return lax.dynamic_index_in_dim(blocks, own ^ distance, 0, keepdims=False)

    received = [exchanged(block(distance), "coef", distance) for distance in range(1, parts)]
    mine = sum(received, block(0))
    distance = 1
    while distance < lax.axis_size("tm"):
        mine = mine + exchanged(mine, "tm", distance)
        distance *= 2
    gathered = [mine] + [exchanged(mine, "coef", distance) for distance in range(1, parts)]
    result = jnp.zeros_like(blocks)
    for distance, part in enumerate(gathered):
        result = lax.dynamic_update_index_in_dim(result, part, own ^ distance, 0)
    return result.reshape(value.shape)


def shards(design, observed, slab_counts, gap_mask, filter_taps, kaula_diag, precond):
    epoch_rows, coef_rows = design.shape
    slabs = lax.axis_size("tm")
    owned_rows = coef_rows // slabs
    owner_index = lax.axis_index("tm")

    tile = LANES if coef_rows % LANES == 0 else owned_rows
    tiles = coef_rows // tile
    width = max(
        -(-(slab + 1) * owned_rows // tile) - slab * owned_rows // tile for slab in range(slabs)
    )
    first_tiles = [min(slab * owned_rows // tile, tiles - width) for slab in range(slabs)]
    window = width * tile
    begins = [first * tile for first in first_tiles]
    begin = jnp.array(begins, jnp.int32)[owner_index]
    offset = owner_index * owned_rows - begin

    pieces = jnp.stack([design[:, start : start + window] for start in begins])
    columns = lax.all_to_all(pieces, "tm", 0, 0).reshape(slabs * epoch_rows, window)

    position = jnp.arange(epoch_rows, dtype=jnp.int32)
    own_weight = ((gap_mask == 1) & (position < slab_counts[0])).astype(jnp.float32)
    columns_count = observed.shape[1]
    weight_rows = own_weight.reshape(-1, columns_count)
    shares = lax.axis_size("coef")
    spare = -(epoch_rows + weight_rows.shape[0]) % (8 * shares)
    packed = jnp.concatenate(
        [observed, weight_rows, jnp.zeros((spare, columns_count), jnp.float32)]
    ).reshape(shares, -1, columns_count)
    share = lax.dynamic_index_in_dim(packed, lax.axis_index("coef"), 0, keepdims=False)
    packed = lax.all_gather(share, ("tm", "coef"), axis=0).reshape(slabs, -1, columns_count)
    observed_all = packed[:, :epoch_rows].reshape(-1, columns_count)
    weight = packed[:, epoch_rows : epoch_rows + weight_rows.shape[0]].reshape(-1, 1)
    lower_block, upper_block = block_pair(filter_taps)

    def weighted(values):
        inner = forward(weight * values, lower_block, upper_block)
        return (weight * backward(inner, lower_block, upper_block)).astype(jnp.bfloat16)

    def transposed(filtered):
        return lax.dot_general(
            columns, filtered, (((0,), (0,)), ((), ())), preferred_element_type=jnp.float32
        )

    def reduced(vector, rows):
        product = jnp.dot(
            columns, vector.astype(jnp.bfloat16), preferred_element_type=jnp.float32
        )
        unit = 8 * lax.axis_size("coef")
        spare = -(product.shape[0] + len(rows)) % unit
        extra = jnp.stack(rows + [jnp.zeros_like(rows[0])] * spare)
        total = total_sum(jnp.concatenate([product, extra]))
        return total[: product.shape[0]], [total[product.shape[0] + i] for i in range(len(rows))]

    local = jnp.arange(window, dtype=jnp.int32)
    owned = (local >= offset) & (local < offset + owned_rows)

    def window_of(values):
        cut = lax.dynamic_slice_in_dim(values, begin, window, 0)
        return jnp.where(owned, cut, 0.0)[:, None]

    kaula_col = window_of(kaula_diag)
    precond_col = window_of(precond)

    residual = transposed(weighted(observed_all))
    solution = jnp.zeros_like(residual)
    direction = None
    for iteration in range(ITERS):
        scaled = precond_col * residual
        rows = [jnp.sum(residual * scaled, 0), jnp.sum(kaula_col * scaled * scaled, 0)]
        if iteration:
            rows.append(jnp.sum(kaula_col * scaled * direction, 0))
        product, sums = reduced(scaled, rows)
        if iteration:
            ratio = sums[0] / norm_now
            direction = scaled + ratio * direction
            slab_values = product + ratio * slab_values
            ridge = sums[1] + 2.0 * ratio * sums[2] + ratio * ratio * ridge
        else:
            direction, slab_values, ridge = scaled, product, sums[1]
        norm_now = sums[0]
        filtered = weighted(slab_values)
        curvature = jnp.sum(slab_values * filtered.astype(jnp.float32), 0) + ridge
        image = transposed(filtered) + kaula_col * direction
        step_len = norm_now / curvature
        solution = solution + step_len * direction
        residual = residual - step_len * image
    return tuple(
        lax.dynamic_slice_in_dim(values, offset, owned_rows, 0) for values in (solution, residual)
    )


def solution(mesh):
    placed = (P("tm", "coef"), P("tm", None), P("tm"), P("tm"), P(), P("coef"), P("coef"))
    return jax.shard_map(
        shards,
        mesh=mesh,
        in_specs=placed,
        out_specs=(P(("coef", "tm"), None), P(("coef", "tm"), None)),
        check_vma=False,
    )
```
